32 devices in a mesh: dp: 4 (over z), expert: 8 (over y, x, core).
Axes of the slice: x: 2, y: 2, z: 4, core: 2. Of those that a mesh axis runs over, the one named last changes fastest.
Arguments:
- tokens: bfloat16 [16384, 1024], P(('dp', 'expert')), may hold values from -6 to 6
- lengths: int32 [32], P(('dp', 'expert')), may hold values from 1 to 512, 12288 in all
- routes: int32 [16384, 1], P(('dp', 'expert')), may hold values from 0 to 7; in each aligned block of 512 rows (0 to 511, 512 to 1023, ...) at most 96 rows name the same one
- cotangent: bfloat16 [16384, 1024], P(('dp', 'expert')), may hold values from -6 to 6
- entry_gain: float32 [1024], P('expert'), may hold values from 0.5 to 1.5
- entry_shift: float32 [1024], P('expert'), may hold values from -1.75 to 1.75
- joint_weight: float32 [1024, 3072], P('expert'), may hold values from -0.1875 to 0.1875
- joint_bias: float32 [2048], P('expert'), may hold values from -1.75 to 1.75
- merge_weight: float32 [1024, 1024], P('expert'), may hold values from -0.75 to 0.75
- merge_bias: float32 [1024], P('expert'), may hold values from -1.75 to 1.75
- second_gain: float32 [1024], P('expert'), may hold values from 0.5 to 1.5
- second_shift: float32 [1024], P('expert'), may hold values from -1.75 to 1.75
- widen_weight: float32 [1024, 4096], P('expert'), may hold values from -0.1875 to 0.1875
- widen_bias: float32 [4096], P('expert'), may hold values from -1.75 to 1.75
- narrow_weight: float32 [4096, 1024], P('expert'), may hold values from -0.09375 to 0.09375
- narrow_bias: float32 [1024], P('expert'), may hold values from -1.75 to 1.75
- router_weight: float32 [1024, 8], P('expert'), may hold values from -0.125 to 0.125
- mixing_weight: float32 [1024, 2], P('expert'), may hold values from -0.1875 to 0.1875
- expert_widen: float32 [8, 1024, 4096], P('expert', 'dp'), may hold values from -0.1875 to 0.1875
- expert_raise: float32 [8, 4096], P('expert', 'dp'), may hold values from -0.625 to 0.625
- expert_narrow: float32 [8, 4096, 1024], P('expert', 'dp'), may hold values from -0.75 to 0.75
- expert_offset: float32 [8, 1024], P('expert', 'dp'), may hold values from -3 to 3
Outputs:
- layer_output: bfloat16 [16384, 1024], P(('dp', 'expert'))
- input_grad: bfloat16 [16384, 1024], P(('dp', 'expert'))
- entry_gain_grad: float32 [1024], P('expert')
- entry_shift_grad: float32 [1024], P('expert')
- joint_weight_grad: float32 [1024, 3072], P('expert')
- joint_bias_grad: float32 [2048], P('expert')
- merge_weight_grad: float32 [1024, 1024], P('expert')
- merge_bias_grad: float32 [1024], P('expert')
- second_gain_grad: float32 [1024], P('expert')
- second_shift_grad: float32 [1024], P('expert')
- widen_weight_grad: float32 [1024, 4096], P('expert')
- widen_bias_grad: float32 [4096], P('expert')
- narrow_weight_grad: float32 [4096, 1024], P('expert')
- narrow_bias_grad: float32 [1024], P('expert')
- router_weight_grad: float32 [1024, 8], P('expert')
- mixing_weight_grad: float32 [1024, 2], P('expert')
- expert_widen_grad: float32 [8, 1024, 4096], P('expert', 'dp')
- expert_raise_grad: float32 [8, 4096], P('expert', 'dp')
- expert_narrow_grad: float32 [8, 4096, 1024], P('expert', 'dp')
- expert_offset_grad: float32 [8, 1024], P('expert', 'dp')
The draws below stay inside these ranges and needn't reach their ends.
Inputs may be any that keep to these rules, and one draw needn't show every extreme that they name: lengths[s] counts the valid rows at the start of sequence s; the longest is exactly 512. `routes`: within the 512 rows of one sequence no expert is named more than 96 times, and in some sequence one expert exactly 96 times.
All inputs are finite; a program needn't handle non-finite values. No bound on the sum of `lengths` on one device may be relied on, other than what follows from the above.
Results may differ from the reference program's by a relative error of at most 0.025.
Values may be sent and summed in bfloat16 or wider, within the bound.
A program may use at most 256 MiB of HBM per device.

```python
import math
import jax
import jax.numpy as jnp
import numpy as np
from jax import lax

D = 1024
HEADS = 16
HEAD_DIM = 64
FF = 4096
FE = 4096
SEQ_LEN = 512
SEQUENCES = 32
TOKENS = 16384
EXPERTS = 8
CAP = 96


def with_spikes(values, stream_key, source, target, parts, factor):
    owner, partner = [(jnp.arange(values.shape[dim]) // (values.shape[dim] // parts)).reshape([-1 if axis == dim else 1 for axis in range(values.ndim)]) for dim in (source, target)]
    chosen = jax.random.permutation(stream_key, parts)[partner]
    strong = (owner == chosen) | (owner == (partner + parts // 2) % parts)
    return jnp.where(strong, factor * values, values)


def level_of(key, shape, cuts, low, high):
    def one(dim, parts):
        steps = jax.random.uniform(jax.random.fold_in(jax.random.fold_in(key, 6), dim), (parts,), jnp.float32, low / len(cuts), high / len(cuts))
        return jnp.repeat(jnp.exp(steps), shape[dim] // parts).reshape((-1,) + (1,) * (len(shape) - dim - 1))

    factor_of = one(*cuts[0])
    for cut in cuts[1:]:
        factor_of = factor_of * one(*cut)
    return factor_of


def split_up(count, total, bound, skew):
    weights = [(1 << 20) // math.isqrt(grade ** skew) + 1 for grade in range(2, count + 1)]
    surplus, holding = total - bound - (count - 1), [1] * (count - 1)
    while surplus > 0:
        free = [i for i in range(count - 1) if holding[i] < bound]
        whole, remaining = sum([weights[i] for i in free]), surplus
        for i in free:
            extra = min(bound - holding[i], max(1, remaining * weights[i] // whole), surplus)
            holding[i] = holding[i] + extra
            surplus = surplus - extra
    return np.array([bound] + holding)


def ragged_sizes(own_key, number_of, total, limit, skew):
    if number_of == 2:
        one = jax.random.randint(own_key, (), max(1, total - limit), min(limit, total - 1) + 1)
        return jnp.stack([one, total - one])
    sizes = jnp.asarray(split_up(number_of, total, limit, skew), jnp.int32)
    couples = (number_of - 1) // 2
    giver, sink = sizes[1:1 + 2 * couples:2], sizes[2:2 + 2 * couples:2]
    room = jnp.minimum(giver - 1, limit - sink)
    shifted = jax.random.randint(jax.random.fold_in(own_key, 1), (couples,), 0, 1 << 20) % (room + 1)
    sizes = sizes.at[1:1 + 2 * couples:2].set(giver - shifted).at[2:2 + 2 * couples:2].set(sink + shifted)
    return sizes[jax.random.permutation(jax.random.fold_in(own_key, 2), number_of)]


def routed_block(stream_key, own, number, rows, count, top, limit, lean):
    sequence = jax.random.permutation(stream_key, count)
    crowded, ordinary = shares(count, rows * top, limit, lean, True), shares(count, rows * top, limit, lean, False)
    places = jnp.arange(count)

    def named(sizes, offset_by):
        used = int((sizes > 0).sum())
        fixed = max(1, used // 4)
        passed = fixed + (places - fixed + offset_by * (used - fixed)) % max(1, count - fixed)
        return jnp.zeros((count,), jnp.int32).at[sequence[jnp.where(places < fixed, places, passed)]].set(jnp.asarray(sizes, jnp.int32))

    sizes = jnp.where(number % 4 == 0, named(crowded, number // 4), named(ordinary, number - number // 4 - 1))
    mixed = jax.random.permutation(jax.random.fold_in(own, 3), count)
    donor, taker = mixed[0:count // 2 * 2:2], mixed[1:count // 2 * 2:2]
    room = jnp.minimum(sizes[donor] - 1, limit - sizes[taker]) // 2
    room = jnp.where((donor == sequence[0]) | (taker == sequence[0]) | (sizes[taker] == 0), 0, jnp.maximum(room, 0))
    passed = jax.random.randint(jax.random.fold_in(own, 4), (count // 2,), 0, 1 << 20) % (room + 1)
    sizes = sizes.at[donor].add(-passed).at[taker].add(passed)
    items = jnp.searchsorted(jnp.cumsum(sizes), jnp.arange(rows * top), side="right").astype(jnp.int32)
    table = items.reshape(top, rows).T
    table = table[jax.random.permutation(jax.random.fold_in(own, 1), rows)]
    offset_by = jax.random.randint(jax.random.fold_in(own, 2), (rows, 1), 0, top)
    return jnp.take_along_axis(table, (jnp.arange(top)[None, :] + offset_by) % top, axis=1)


def shares(number_of, total, limit, lean, full):
    weights = [(1 << 20) // math.isqrt(grade ** lean) + 1 for grade in range(1, number_of + 1)]
    largest = limit if full else min(limit, max(-(-total // number_of), total * weights[0] // sum(weights)))
    least = 1 if total - largest >= number_of - 1 else 0
    given, surplus = [largest] + [least] * (number_of - 1), total - largest - least * (number_of - 1)
    while surplus > 0:
        movable = [i for i in range(1, number_of) if given[i] < largest] or [i for i in range(1, number_of) if given[i] < limit]
        whole, left = sum([weights[i] for i in movable]), surplus
        for i in movable:
            addition = min(limit - given[i], max(1, left * weights[i] // whole), surplus)
            given[i] = given[i] + addition
            surplus = surplus - addition
    return np.array(given)


def normal_values(stream_key, extent, scale, most, shards=(), kind=jnp.bfloat16):
    result = jax.random.normal(stream_key, extent, jnp.float32) * scale
    if len(shards) > 0:
        result = level_of(stream_key, extent, shards, -0.22, 0.18) * result
    return jnp.clip(result, min=-most, max=most).astype(kind)


def heavy_noise(rng, shape, scale, most, cuts, heavy, held_as=jnp.bfloat16):
    result = scale * jax.random.normal(rng, shape, jnp.float32)
    if cuts:
        result = result * level_of(rng, shape, cuts, -0.22, 0.18)
    return jnp.clip(with_spikes(result, jax.random.fold_in(rng, 3), *heavy), -most, most).astype(held_as)


def setup_inputs(seed: int = 0) -> dict:
    splits = jax.random.split(jax.random.key(seed), 23)
    tokens = normal_values(splits[0], (TOKENS, D), 1.0, 6.0, ((0, 32),))
    lengths = ragged_sizes(splits[1], SEQUENCES, SEQUENCES * SEQ_LEN * 3 // 4, SEQ_LEN, 1).astype(jnp.int32)
    routes_keys = jax.random.split(jax.random.fold_in(splits[2], 1), TOKENS // SEQ_LEN)
    routes_turns = jax.random.permutation(jax.random.fold_in(splits[2], 3), TOKENS // SEQ_LEN)
    routes = jax.vmap(lambda own, number: routed_block(jax.random.fold_in(splits[2], 2), own, number, SEQ_LEN, EXPERTS, 1, CAP, 2))(routes_keys, routes_turns).reshape((TOKENS, 1))
    cotangent = heavy_noise(splits[3], (TOKENS, D), 1.0, 6.0, ((0, 32),), (0, 1, 32, 2.75))
    entry_gain = jnp.clip(1.0 + 0.1 * jax.random.normal(splits[4], (D,), jnp.float32), 0.5, 1.5)
    entry_shift = normal_values(splits[5], (D,), 0.3, 1.75, ((0, 8),), jnp.float32)
    joint_weight = normal_values(splits[6], (D, 3 * D), D ** -0.5, 0.1875, ((0, 8),), jnp.float32)
    joint_bias = normal_values(splits[7], (2 * D,), 0.3, 1.75, ((0, 8),), jnp.float32)
    merge_weight = normal_values(splits[8], (D, D), (D // 16) ** -0.5, 0.75, ((0, 8),), jnp.float32)
    merge_bias = normal_values(splits[9], (D,), 0.3, 1.75, ((0, 8),), jnp.float32)
    second_gain = jnp.clip(1.0 + 0.1 * jax.random.normal(splits[10], (D,), jnp.float32), 0.5, 1.5)
    second_shift = normal_values(splits[11], (D,), 0.3, 1.75, ((0, 8),), jnp.float32)
    widen_weight = normal_values(splits[12], (D, FF), D ** -0.5, 0.1875, ((0, 8),), jnp.float32)
    widen_bias = normal_values(splits[13], (FF,), 0.3, 1.75, ((0, 8),), jnp.float32)
    narrow_weight = normal_values(splits[14], (FF, D), FF ** -0.5, 0.09375, ((0, 8),), jnp.float32)
    narrow_bias = normal_values(splits[15], (D,), 0.3, 1.75, ((0, 8),), jnp.float32)
    router_weight = normal_values(splits[16], (D, EXPERTS), (2 * D) ** -0.5, 0.125, ((0, 8),), jnp.float32)
    mixing_weight = normal_values(splits[17], (D, 2), D ** -0.5, 0.1875, ((0, 8),), jnp.float32)
    expert_widen = normal_values(splits[18], (EXPERTS, D, FE), D ** -0.5, 0.1875, ((0, 8), (1, 4)), jnp.float32)
    expert_raise = normal_values(splits[19], (EXPERTS, FE), 0.1, 0.625, ((0, 8), (1, 4)), jnp.float32)
    expert_narrow = normal_values(splits[20], (EXPERTS, FE, D), (max(1, FE // (EXPERTS * EXPERTS))) ** -0.5, 0.75, ((0, 8), (1, 4)), jnp.float32)
    expert_offset = normal_values(splits[21], (EXPERTS, D), (EXPERTS / 16), 3.0, ((0, 8), (1, 4)), jnp.float32)
    return {"tokens": tokens, "lengths": lengths, "routes": routes, "cotangent": cotangent, "entry_gain": entry_gain, "entry_shift": entry_shift, "joint_weight": joint_weight, "joint_bias": joint_bias, "merge_weight": merge_weight, "merge_bias": merge_bias, "second_gain": second_gain, "second_shift": second_shift, "widen_weight": widen_weight, "widen_bias": widen_bias, "narrow_weight": narrow_weight, "narrow_bias": narrow_bias, "router_weight": router_weight, "mixing_weight": mixing_weight, "expert_widen": expert_widen, "expert_raise": expert_raise, "expert_narrow": expert_narrow, "expert_offset": expert_offset}


@jax.custom_vjp
def low(v):
    return lax.optimization_barrier(v.astype(jnp.bfloat16)).astype(jnp.float32)

@jax.custom_vjp
def low_back(v):
    return v

def low_keep(v):
    return (low(v), None)

def low_pass(kept, grad):
    return (grad,)

def back_keep(v):
    return (v, None)

def back_low(kept, grad):
    return (low(grad),)
low.defvjp(low_keep, low_pass)
low_back.defvjp(back_keep, back_low)
EPSILON = 1e-05
FLOOR = -1e+30
HIGHEST = lax.Precision.HIGHEST

def matmul(left, right):
    return jnp.dot(left, right, precision=HIGHEST)

def layer_norm(values, gain, shift):
    centred = values - lax.optimization_barrier(jnp.mean(values, axis=-1, keepdims=True))
    spread = lax.optimization_barrier(jnp.mean(centred * centred, axis=-1, keepdims=True))
    return centred * lax.rsqrt(spread + EPSILON) * gain + shift

def softmax_rows(logits):
    highest = lax.optimization_barrier(jnp.max(logits, axis=-1, keepdims=True))
    raised = jnp.exp(logits - highest)
    return raised / lax.optimization_barrier(jnp.sum(raised, axis=-1, keepdims=True))

def gelu_tanh(values):
    return jax.nn.gelu(values, approximate=True)

def attend(pieces):
    query, keys, values, length = pieces
    seq = query.shape[0]
    scale = HEAD_DIM ** (-0.5)
    raw = jnp.einsum('qhd,khd->hqk', query, keys, precision=HIGHEST)
    scores = low_back(raw * scale)
    position = jnp.arange(seq, dtype=jnp.int32)
    allowed = (position[None, :] <= position[:, None]) & (position[None, :] < length)
    scores = jnp.where(allowed[None], scores, FLOOR)
    weights = softmax_rows(scores)
    return jnp.einsum('hqk,khd->qhd', low(weights), values, precision=HIGHEST)

def expert_run(pieces):
    rows, lift, lift_add, lower, lower_add = pieces
    raised = low_back(matmul(rows, lift) + lift_add)
    return matmul(low(gelu_tanh(raised)), lower) + lower_add

def reference(tokens, lengths, routes, cotangent, entry_gain, entry_shift, joint_weight, joint_bias, merge_weight, merge_bias, second_gain, second_shift, widen_weight, widen_bias, narrow_weight, narrow_bias, router_weight, mixing_weight, expert_widen, expert_raise, expert_narrow, expert_offset):
    sequences = lengths.shape[0]
    seq = tokens.shape[0] // sequences
    width = tokens.shape[1]
    experts = router_weight.shape[1]
    capacity = CAP
    slots = sequences * capacity
    position = jnp.tile(jnp.arange(seq, dtype=jnp.int32), sequences)
    owner = jnp.repeat(jnp.arange(sequences, dtype=jnp.int32), seq)
    valid_rows = position < lengths[owner]
    valid_int = valid_rows.astype(jnp.int32)
    route = routes[:, 0]
    route_match = route[:, None] == jnp.arange(experts, dtype=jnp.int32)[None, :]
    chosen = route_match.astype(jnp.int32) * valid_int[:, None]
    counted = jnp.cumsum(chosen.reshape(sequences, seq, experts), axis=1).reshape(-1, experts)
    placed = lax.optimization_barrier(jnp.sum(chosen * counted, axis=1)) - 1
    slot_index = (route * slots + owner * capacity + placed).astype(jnp.int32)
    target = jnp.where(valid_rows, slot_index, experts * slots).astype(jnp.int32)
    fetch = jnp.where(valid_rows, slot_index, 0).astype(jnp.int32)
    valid = valid_rows.astype(jnp.float32)[:, None]
    route_hot = route_match.astype(jnp.float32)

    def forward(inputs, gain_one, shift_one, joint, joint_add, merge, merge_add, gain_two, shift_two, widen, widen_add, narrow, narrow_add, router, mixing, lift, lift_add, lower, lower_add):
        gain_one = low(gain_one)
        shift_one = low(shift_one)
        joint = low(joint)
        joint_add = low(joint_add)
        merge = low(merge)
        merge_add = low(merge_add)
        gain_two = low(gain_two)
        shift_two = low(shift_two)
        widen = low(widen)
        widen_add = low(widen_add)
        narrow = low(narrow)
        narrow_add = low(narrow_add)
        router = low(router)
        mixing = low(mixing)
        lift = low(lift)
        lift_add = low(lift_add)
        lower = low(lower)
        lower_add = low(lower_add)
        normed = low(layer_norm(inputs, gain_one, shift_one))
        bias_full = jnp.concatenate([joint_add[:width], jnp.zeros((width,), jnp.float32), joint_add[width:]])
        projected = low_back(low(matmul(normed, joint) + bias_full))
        query = projected[:, :width].reshape(sequences, seq, HEADS, HEAD_DIM)
        keys = projected[:, width:2 * width].reshape(sequences, seq, HEADS, HEAD_DIM)
        values = projected[:, 2 * width:].reshape(sequences, seq, HEADS, HEAD_DIM)
        context = lax.map(jax.checkpoint(attend), (query, keys, values, lengths))
        context = low_back(low(context.reshape(-1, width)))
        residual = inputs + low_back(matmul(context, merge) + merge_add)
        hidden = low(layer_norm(residual, gain_two, shift_two))
        active = low(gelu_tanh(low_back(matmul(hidden, widen) + widen_add)))
        dense = low_back(matmul(active, narrow) + narrow_add)
        gate = lax.optimization_barrier(jnp.sum(softmax_rows(low_back(matmul(hidden, router))) * route_hot, axis=-1, keepdims=True))
        blend = softmax_rows(low_back(matmul(hidden, mixing)))
        buffer = jnp.zeros((experts * slots, width), jnp.float32).at[target].add(hidden, mode='drop')
        buffer = low_back(buffer.reshape(experts, slots, width))
        produced = lax.map(jax.checkpoint(expert_run), (buffer, lift, lift_add, lower, lower_add))
        produced = low_back(low(produced)).reshape(experts * slots, width)
        combined = produced[fetch] * valid
        return valid * (residual + blend[:, 0:1] * dense + blend[:, 1:2] * gate * combined)
    output, backward = jax.vjp(forward, tokens.astype(jnp.float32), entry_gain, entry_shift, joint_weight, joint_bias, merge_weight, merge_bias, second_gain, second_shift, widen_weight, widen_bias, narrow_weight, narrow_bias, router_weight, mixing_weight, expert_widen, expert_raise, expert_narrow, expert_offset)
    grads = backward(cotangent.astype(jnp.float32))
    return (output.astype(jnp.bfloat16), grads[0].astype(jnp.bfloat16), grads[1], grads[2], grads[3], grads[4], grads[5], grads[6], grads[7], grads[8], grads[9], grads[10], grads[11], grads[12], grads[13], grads[14], grads[15], grads[16], grads[17], grads[18])
```

```python
import jax
import jax.numpy as jnp
from jax import lax
from jax.sharding import PartitionSpec as P

HEADS = 16
HEAD_DIM = 64


EPSILON = 1e-05
FLOOR = -1e30


def layer_norm(values, gain, shift):
    centred = values - jnp.mean(values, axis=-1, keepdims=True)
    spread = jnp.mean(centred * centred, axis=-1, keepdims=True)
    return centred * lax.rsqrt(spread + EPSILON) * gain + shift


def softmax_rows(logits):
    highest = jnp.max(logits, axis=-1, keepdims=True)
    raised = jnp.exp(logits - highest)
    return raised / jnp.sum(raised, axis=-1, keepdims=True)


def gelu_tanh(values):
    return jax.nn.gelu(values, approximate=True)


def product(left, right):
    return jnp.dot(left, right, preferred_element_type=jnp.float32)


def product_left(left, right):
    return lax.dot_general(
        left, right, (((0,), (0,)), ((), ())), preferred_element_type=jnp.float32
    )


def product_right(left, right):
    return lax.dot_general(
        left, right, (((1,), (1,)), ((), ())), preferred_element_type=jnp.float32
    )


def column_sums(values):
    return jnp.sum(values.astype(jnp.float32), axis=0)


CHUNKS = 2


def swap(bit, size):
    return [(i, i ^ bit) for i in range(size)]


def add_low(*terms):
    total = terms[0].astype(jnp.float32)
    for term in terms[1:]:
        total = total + term.astype(jnp.float32)
    return total.astype(jnp.bfloat16)


def pick(array, index):
    return lax.dynamic_index_in_dim(array, index, 0, keepdims=False)


def gather_rows(shard):
    size = lax.axis_size("expert")
    if size != 8:
        return lax.all_gather(shard, "expert", axis=0, tiled=True)
    me = lax.axis_index("expert")
    half = shard.shape[0] // 2
    from_x = lax.ppermute(shard, "expert", swap(2, 8))
    from_y = lax.ppermute(shard, "expert", swap(4, 8))
    first = lax.ppermute(from_y[:half], "expert", swap(2, 8))
    second = lax.ppermute(from_x[half:], "expert", swap(4, 8))
    mine = jnp.stack([shard, from_x, from_y, jnp.concatenate([first, second])])
    other = lax.ppermute(mine, "expert", swap(1, 8))
    whole = jnp.zeros((8,) + shard.shape, shard.dtype)
    for i in range(4):
        whole = lax.dynamic_update_index_in_dim(whole, mine[i], me ^ (2 * i), 0)
        whole = lax.dynamic_update_index_in_dim(whole, other[i], me ^ (2 * i + 1), 0)
    return whole.reshape((8 * shard.shape[0],) + shard.shape[1:])


def scatter_rows(grads):
    size = lax.axis_size("expert")
    if size != 8:
        return lax.psum_scatter(grads, "expert", scatter_dimension=0, tiled=True)
    me = lax.axis_index("expert")
    core = me & 1
    chip = me // 2
    rows = grads.shape[0] // 8
    half = rows // 2
    parts = grads.reshape((4, 2, rows) + grads.shape[1:])
    sent = lax.dynamic_index_in_dim(parts, 1 - core, 1, keepdims=False)
    kept = lax.dynamic_index_in_dim(parts, core, 1, keepdims=False)
    both = add_low(kept, lax.ppermute(sent, "expert", swap(1, 8)))
    far = pick(both, chip ^ 3)
    by_x = lax.ppermute(far[:half], "expert", swap(2, 8))
    by_y = lax.ppermute(far[half:], "expert", swap(4, 8))
    to_x = pick(both, chip ^ 1)
    to_y = pick(both, chip ^ 2)
    to_x = jnp.concatenate([to_x[:half], add_low(to_x[half:], by_y)])
    to_y = jnp.concatenate([add_low(to_y[:half], by_x), to_y[half:]])
    from_x = lax.ppermute(to_x, "expert", swap(2, 8))
    from_y = lax.ppermute(to_y, "expert", swap(4, 8))
    return add_low(pick(both, chip), from_x, from_y)


def sum_planes(part):
    if lax.axis_size("dp") != 4:
        return lax.psum(part, "dp")
    plane = lax.axis_index("dp")
    inner = (plane == 1) | (plane == 2)
    pair = lax.optimization_barrier(add_low(part, lax.ppermute(part, "dp", [(0, 1), (3, 2)])))
    total = lax.optimization_barrier(
        add_low(pair, lax.ppermute(pair, "dp", [(1, 2), (2, 1)]))
    )
    return jnp.where(inner, total, lax.ppermute(total, "dp", [(1, 0), (2, 3)]))


def per_device(
    tokens,
    lengths,
    routes,
    cotangent,
    entry_gain,
    entry_shift,
    joint_weight,
    joint_bias,
    merge_weight,
    merge_bias,
    second_gain,
    second_shift,
    widen_weight,
    widen_bias,
    narrow_weight,
    narrow_bias,
    router_weight,
    mixing_weight,
    expert_widen,
    expert_raise,
    expert_narrow,
    expert_offset,
):
    single = jnp.float32
    brain = jnp.bfloat16
    seq, width = tokens.shape
    experts = lax.axis_size("expert")
    planes = lax.axis_size("dp")
    chunks = CHUNKS
    rows = width // experts
    hidden_width = widen_weight.shape[1]
    inner_width = expert_widen.shape[2]
    own_inner = inner_width // planes
    piece = own_inner // chunks

    def columns(vector):
        return vector.reshape(-1, rows).T

    def spread(lines):
        count = lines.shape[0]
        return lines.reshape(count, experts, rows).transpose(1, 0, 2).reshape(count * width)

    def unspread(vector):
        count = vector.shape[0] // width
        return vector.reshape(experts, count, rows).transpose(1, 0, 2).reshape(count, width)

    bias_lines = joint_bias.shape[0] // rows
    widen_lines = widen_bias.shape[0] // rows
    lines = 6 + bias_lines + widen_lines
    small = jnp.concatenate(
        [
            columns(entry_gain),
            columns(entry_shift),
            columns(merge_bias),
            columns(second_gain),
            columns(second_shift),
            columns(narrow_bias),
            columns(joint_bias),
            columns(widen_bias),
            router_weight,
            mixing_weight,
        ],
        axis=1,
    )
    used = small.shape[1]
    padding = -used % 128
    small = jnp.pad(small, ((0, 0), (0, padding)))
    first_pack = jnp.concatenate([joint_weight, merge_weight, small], axis=1).astype(brain)
    first = gather_rows(first_pack)
    joint = first[:, : 3 * width]
    merge = first[:, 3 * width : 4 * width]
    little = first[:, 4 * width :]
    across = little[:, :lines].astype(single).T
    gain_one, shift_one, merge_add, gain_two, shift_two, narrow_add = [across[i] for i in range(6)]
    joint_add = spread(across[6 : 6 + bias_lines])
    widen_add = spread(across[6 + bias_lines : lines])
    router = little[:, lines : lines + experts]
    mixing = little[:, lines + experts : lines + experts + 2]
    widen = gather_rows(widen_weight.astype(brain))
    narrow = gather_rows(narrow_weight.astype(brain))

    offsets = jnp.concatenate([expert_raise[0], expert_offset[0]]).astype(brain)
    offsets = lax.all_gather(offsets, "dp", axis=0, tiled=False).astype(single)
    lift_add = offsets[:, :own_inner].reshape(planes, chunks, piece)
    lower_add = offsets[:, own_inner:].reshape(width)
    lift_local = expert_widen[0].astype(brain).reshape(-1, planes, chunks, piece)
    lower_local = expert_narrow[0].astype(brain).reshape(chunks, piece, width)
    lifts, lowers = [], []
    for c in range(chunks):
        lifts.append(
            lax.all_gather(
                lift_local[:, :, c].reshape(-1, planes * piece), "dp", axis=0, tiled=True
            )
        )
        lowers.append(lax.all_gather(lower_local[c], "dp", axis=0, tiled=True))

    heads = HEADS
    head_size = HEAD_DIM
    scale = head_size ** (-0.5)
    capacity = seq * 3 // (2 * experts)
    inputs = tokens.astype(single)
    position = jnp.arange(seq, dtype=jnp.int32)
    length = lengths[0]
    valid_rows = position < length
    valid = valid_rows.astype(single)[:, None]
    normed, norm_one_back = jax.vjp(layer_norm, inputs, gain_one, shift_one)
    normed_low = normed.astype(brain)
    bias_full = jnp.concatenate([joint_add[:width], jnp.zeros((width,), single), joint_add[width:]])
    projected = (product(normed_low, joint) + bias_full).astype(brain)
    query = projected[:, :width].reshape(seq, heads, head_size)
    keys = projected[:, width : 2 * width].reshape(seq, heads, head_size)
    values = projected[:, 2 * width :].reshape(seq, heads, head_size)
    allowed = (position[None, :] <= position[:, None]) & (position[None, :] < length)

    def score_block():
        raw = jnp.einsum("qhd,khd->hqk", query, keys, preferred_element_type=single) * scale
        return jnp.where(allowed[None], raw, FLOOR)

    scores = score_block()
    highest = jnp.max(scores, axis=-1, keepdims=True)
    expanded = jnp.exp(scores - highest)
    totals = jnp.sum(expanded, axis=-1, keepdims=True)
    log_total = highest + jnp.log(totals)
    weights_low = (expanded / totals).astype(brain)
    context = (
        jnp.einsum("hqk,khd->qhd", weights_low, values, preferred_element_type=single)
        .reshape(seq, width)
        .astype(brain)
    )
    residual = inputs + product(context, merge) + merge_add
    hidden_norm, norm_two_back = jax.vjp(layer_norm, residual, gain_two, shift_two)
    hidden = hidden_norm.astype(brain)

    route = routes[:, 0]
    expert_ids = jnp.arange(experts, dtype=jnp.int32)
    route_match = route[:, None] == expert_ids[None, :]
    route_hot = route_match.astype(single)

    def gating(logit_rows, mixing_rows):
        gate_rows = jnp.sum(softmax_rows(logit_rows) * route_hot, axis=-1, keepdims=True)
        return (gate_rows, softmax_rows(mixing_rows))

    (gate, blend), gating_back = jax.vjp(gating, product(hidden, router), product(hidden, mixing))
    chosen = route_match.astype(jnp.int32) * valid_rows.astype(jnp.int32)[:, None]
    placed = jnp.sum(chosen * jnp.cumsum(chosen, axis=0), axis=1) - 1
    target = jnp.where(valid_rows, route * capacity + placed, -1)
    slot_ids = jnp.arange(experts * capacity, dtype=jnp.int32)
    placer = (slot_ids[:, None] == target[None, :]).astype(brain)

    def exchange(slots):
        return lax.all_to_all(
            slots.reshape(experts, capacity, width),
            "expert",
            split_axis=0,
            concat_axis=0,
            tiled=True,
        ).reshape(experts * capacity, width)

    arrived = exchange(product(placer, hidden).astype(brain))
    grad_out = valid * cotangent.astype(single)
    grad_combined = (blend[:, 1:2] * gate * grad_out).astype(brain)
    grad_arrived = exchange(product(placer, grad_combined).astype(brain))

    widened = product(hidden, widen) + widen_add
    active, active_back = jax.vjp(gelu_tanh, widened)
    active_low = active.astype(brain)
    dense = product(active_low, narrow) + narrow_add
    grad_dense = (blend[:, 0:1] * grad_out).astype(brain)
    grad_narrow = product_left(active_low, grad_dense).astype(brain)
    grad_narrow_add = column_sums(grad_dense)
    grad_widened = active_back(product_right(grad_dense, narrow))[0].astype(brain)
    grad_widen = product_left(hidden, grad_widened).astype(brain)
    grad_widen_add = column_sums(grad_widened)
    grad_hidden_dense = product_right(grad_widened, widen)
    narrow_out = sum_planes(scatter_rows(grad_narrow)).astype(single)
    widen_out = sum_planes(scatter_rows(grad_widen)).astype(single)

    produced = lower_add
    grad_rows = 0.0
    lift_outs, lower_outs, lift_add_parts = [], [], []
    for c in range(chunks):
        lift, lower = lifts[c], lowers[c]
        raised = product(arrived, lift) + lift_add[:, c].reshape(planes * piece)
        expert_act, expert_back = jax.vjp(gelu_tanh, raised)
        act_low = expert_act.astype(brain)
        produced = produced + product(act_low, lower)
        grad_raised = expert_back(product_right(grad_arrived, lower))[0].astype(brain)
        grad_rows = grad_rows + product_right(grad_raised, lift)
        grad_lower = product_left(act_low, grad_arrived).astype(brain)
        grad_lift = product_left(arrived, grad_raised).astype(brain)
        lower_outs.append(
            lax.psum_scatter(grad_lower, "dp", scatter_dimension=0, tiled=True).astype(single)
        )
        lift_outs.append(
            lax.psum_scatter(grad_lift, "dp", scatter_dimension=0, tiled=True).astype(single)
        )
        lift_add_parts.append(column_sums(grad_raised).reshape(planes, piece))
    returned = exchange(produced.astype(brain))
    grad_returned = exchange(grad_rows.astype(brain))
    offset_grads = jnp.concatenate(
        lift_add_parts + [column_sums(grad_arrived).reshape(planes, -1)], axis=1
    ).astype(brain)
    offset_sum = lax.psum_scatter(offset_grads, "dp", scatter_dimension=0, tiled=True).astype(single)
    lift_add_sum = offset_sum[:, :own_inner]
    lower_add_sum = offset_sum[:, own_inner:]
    lift_sum = jnp.stack(
        [out.reshape(-1, planes, piece) for out in lift_outs], axis=2
    ).reshape(expert_widen.shape)
    lower_sum = jnp.concatenate(lower_outs, axis=0)[None]

    combined = product_left(placer, returned)
    mixture = gate * combined
    output = valid * (residual + blend[:, 0:1] * dense + blend[:, 1:2] * mixture)
    grad_blend = jnp.concatenate(
        [
            jnp.sum(grad_out * dense, axis=-1, keepdims=True),
            jnp.sum(grad_out * mixture, axis=-1, keepdims=True),
        ],
        axis=1,
    )
    grad_gate = blend[:, 1:2] * jnp.sum(grad_out * combined, axis=-1, keepdims=True)
    grad_logits, grad_mixing = gating_back((grad_gate, grad_blend))
    grad_logits = grad_logits.astype(brain)
    grad_mixing = grad_mixing.astype(brain)
    grad_router = product_left(hidden, grad_logits)
    grad_mixer = product_left(hidden, grad_mixing)
    grad_hidden = (
        product_left(placer, grad_returned)
        + grad_hidden_dense
        + product_right(grad_logits, router)
        + product_right(grad_mixing, mixing)
    )
    grad_residual, grad_gain_two, grad_shift_two = norm_two_back(grad_hidden)
    grad_residual = grad_residual + grad_out
    grad_merged = grad_residual.astype(brain)
    grad_merge = product_left(context, grad_merged)
    grad_merge_add = column_sums(grad_merged)
    grad_context = product_right(grad_merged, merge).astype(brain).reshape(seq, heads, head_size)
    again = jnp.exp(score_block() - log_total)
    again_low = again.astype(brain)
    grad_values = jnp.einsum("hqk,qhd->khd", again_low, grad_context, preferred_element_type=single)
    grad_weights = jnp.einsum("qhd,khd->hqk", grad_context, values, preferred_element_type=single)
    grad_scores = (
        again * (grad_weights - jnp.sum(again * grad_weights, axis=-1, keepdims=True))
    ).astype(brain)
    grad_query = (
        jnp.einsum("hqk,khd->qhd", grad_scores, keys, preferred_element_type=single) * scale
    )
    grad_keys = (
        jnp.einsum("hqk,qhd->khd", grad_scores, query, preferred_element_type=single) * scale
    )
    grad_projected = jnp.concatenate(
        [
            grad_query.reshape(seq, width),
            grad_keys.reshape(seq, width),
            grad_values.reshape(seq, width),
        ],
        axis=1,
    ).astype(brain)
    grad_joint = product_left(normed_low, grad_projected)
    grad_joint_add = jnp.concatenate(
        [column_sums(grad_projected[:, :width]), column_sums(grad_projected[:, 2 * width :])]
    )
    grad_inputs, grad_gain_one, grad_shift_one = norm_one_back(product_right(grad_projected, joint))
    input_grad = (grad_residual + grad_inputs).astype(brain)

    across = jnp.concatenate(
        [
            jnp.stack(
                [
                    grad_gain_one,
                    grad_shift_one,
                    grad_merge_add,
                    grad_gain_two,
                    grad_shift_two,
                    grad_narrow_add,
                ]
            ),
            unspread(grad_joint_add),
            unspread(grad_widen_add),
        ]
    )
    little = jnp.pad(
        jnp.concatenate([across.T, grad_router, grad_mixer], axis=1), ((0, 0), (0, padding))
    )
    last_pack = jnp.concatenate(
        [grad_joint.astype(brain), grad_merge.astype(brain), little.astype(brain)], axis=1
    )
    last = sum_planes(scatter_rows(last_pack)).astype(single)
    little = last[:, 4 * width :]
    across = little[:, :lines].T
    return (
        output.astype(brain),
        input_grad,
        across[0],
        across[1],
        last[:, : 3 * width],
        across[6 : 6 + bias_lines].reshape(-1),
        last[:, 3 * width : 4 * width],
        across[2],
        across[3],
        across[4],
        widen_out,
        across[6 + bias_lines : lines].reshape(-1),
        narrow_out,
        across[5],
        little[:, lines : lines + experts],
        little[:, lines + experts : lines + experts + 2],
        lift_sum,
        lift_add_sum,
        lower_sum,
        lower_add_sum,
    )


def solution(mesh):
    placed = (
        P(("dp", "expert"), None),
        P(("dp", "expert")),
        P(("dp", "expert"), None),
        P(("dp", "expert"), None),
        P("expert"),
        P("expert"),
        P("expert", None),
        P("expert"),
        P("expert", None),
        P("expert"),
        P("expert"),
        P("expert"),
        P("expert", None),
        P("expert"),
        P("expert", None),
        P("expert"),
        P("expert", None),
        P("expert", None),
        P("expert", "dp", None),
        P("expert", "dp"),
        P("expert", "dp", None),
        P("expert", "dp"),
    )
    return jax.shard_map(
        per_device,
        mesh=mesh,
        in_specs=placed,
        out_specs=(
            P(("dp", "expert"), None),
            P(("dp", "expert"), None),
            P("expert"),
            P("expert"),
            P("expert", None),
            P("expert"),
            P("expert", None),
            P("expert"),
            P("expert"),
            P("expert"),
            P("expert", None),
            P("expert"),
            P("expert", None),
            P("expert"),
            P("expert", None),
            P("expert", None),
            P("expert", "dp", None),
            P("expert", "dp"),
            P("expert", "dp", None),
            P("expert", "dp"),
        ),
        check_vma=False,
    )
```
